32 devices in a mesh: samp: 4 (over z), atom: 8 (over y, x, core).
Axes of the slice: x: 2, y: 2, z: 4, core: 2. Of those that a mesh axis runs over, the one named last changes fastest.
Arguments:
- atom_state: bfloat16 [16, 2560, 128], P('samp', 'atom'), may hold values from -6 to 6, as said below
- atom_token: int32 [2560], P('atom'), may hold values from 0 to 319, never falling along the last dimension, each value on 1 to 24 neighbouring positions
- window_valid: int32 [80], P('atom'), may hold values from 1 to 32
- attend_gain: float32 [128], replicated, may hold values from 0.25 to 1.75
- project_weight: bfloat16 [128, 384], replicated, may hold values from -4 to 4
- output_weight: bfloat16 [128, 128], replicated, may hold values from -1.5 to 1.5
- token_bias: float32 [4], replicated, may hold values from -2 to 2
- transit_gain: float32 [128], replicated, may hold values from 0.25 to 1.75
- transit_weight: bfloat16 [128, 512], replicated, may hold values from -0.5 to 0.5
- return_weight: bfloat16 [256, 128], replicated, may hold values from -0.375 to 0.375
- cotangent: bfloat16 [16, 2560, 128], P('samp', 'atom'), may hold values from -6 to 6
Outputs:
- block_out: bfloat16 [16, 2560, 128], P('samp', 'atom')
- state_grad: bfloat16 [16, 2560, 128], P('samp', 'atom')
- grad_attend_gain: float32 [128], replicated
- grad_project: float32 [128, 384], replicated
- grad_output: float32 [128, 128], replicated
- grad_bias: float32 [4], replicated
- grad_transit_gain: float32 [128], replicated
- grad_transit: float32 [128, 512], replicated
- grad_return: float32 [256, 128], replicated
The draws below stay inside these ranges and needn't reach their ends.
Inputs may be any that keep to these rules, and one draw needn't show every extreme that they name: atom_state is finite. `atom_token`: tokens are numbered in order along the atoms; a token has 1 to 24 atoms.
All inputs are finite; a program needn't handle non-finite values.
Results may differ from the reference program's by a relative error of at most 0.025.
The reference program's roundings to bfloat16 on the way (of `normed`, `projected`, `attended`, `residual`, `transit_in`, `gated`, `back_hidden` and `back_res16`) count: a program that leaves them out, or rounds other values in their place, can miss the bound.
Values may be sent and summed in bfloat16 or wider, within the bound.
A program may use at most 64 MiB of HBM per device.

```python
import math
import jax
import jax.numpy as jnp
import numpy as np
from jax import lax

WIDTH = 128
HEADS = 4
TRANS = 256
QWIN = 32
KWIN = 128
HALO = 48
SAMPLES = 16
ATOMS = 2560
WINDOWS = 80
TOKENS = 320


def draw_atom_state(key, part):
    extent = (SAMPLES, ATOMS, WIDTH)
    values = jnp.clip(jax.random.normal(jax.random.fold_in(key, 15), extent, jnp.float32), -6.0, 6.0)
    return values.astype(jnp.bfloat16)


def draw_project_weight(key, part):
    base = jnp.clip(jax.random.normal(jax.random.fold_in(key, 21), (WIDTH, 3 * WIDTH), jnp.float32), -6.0, 6.0)
    base = base / jnp.sqrt(float(WIDTH))
    return base.astype(jnp.bfloat16)


def with_ends(array, own_key, low, high):
    place = [jax.random.randint(jax.random.fold_in(own_key, axis), (), 0, length) for axis, length in enumerate(array.shape)]
    main_axis = array.shape.index(max(array.shape))
    next_to = place[:main_axis] + [(place[main_axis] + 1) % array.shape[main_axis]] + place[main_axis + 1:]
    return array.at[tuple(place)].set(low).at[tuple(next_to)].set(high)


def steps_of(key, dims, split, smallest, largest):
    factor_of, own = 1.0, jax.random.fold_in(key, 6)
    for dim, parts in split:
        heights = jnp.exp(jax.random.uniform(jax.random.fold_in(own, dim), (parts,), jnp.float32, smallest / len(split), largest / len(split)))
        factor_of = factor_of * jnp.repeat(heights, dims[dim] // parts).reshape([-1 if axis == dim else 1 for axis in range(len(dims))])
    return factor_of


def split_up(number_of, total, reach, slope):
    loads = [(1 << 20) // math.isqrt(rank ** slope) + 1 for rank in range(2, number_of + 1)]
    spare, holding = total - reach - (number_of - 1), [1] * (number_of - 1)
    while spare > 0:
        candidates = [i for i in range(number_of - 1) if holding[i] < reach]
        mass, remaining = sum([loads[i] for i in candidates]), spare
        for i in candidates:
            more = min(reach - holding[i], max(1, remaining * loads[i] // mass), spare)
            holding[i] = holding[i] + more
            spare = spare - more
    return np.array([reach] + holding)


def ragged_sizes(own_key, count, total, limit, skew):
    if count == 2:
        one = jax.random.randint(own_key, (), max(1, total - limit), min(limit, total - 1) + 1)
        return jnp.stack([one, total - one])
    tallies = jnp.asarray(split_up(count, total, limit, skew), jnp.int32)
    twos = (count - 1) // 2
    donor, sink = tallies[1:1 + 2 * twos:2], tallies[2:2 + 2 * twos:2]
    margin = jnp.minimum(donor - 1, limit - sink)
    moved = jax.random.randint(jax.random.fold_in(own_key, 1), (twos,), 0, 1 << 20) % (margin + 1)
    tallies = tallies.at[1:1 + 2 * twos:2].set(donor - moved).at[2:2 + 2 * twos:2].set(sink + moved)
    return tallies[jax.random.permutation(jax.random.fold_in(own_key, 2), count)]


def bell_draw(stream_key, shape, scale, most, cuts=(), dtype=jnp.bfloat16):
    values = jax.random.normal(stream_key, shape, jnp.float32) * scale
    if len(cuts) > 0:
        values = steps_of(stream_key, shape, cuts, -0.22, 0.18) * values
    return jnp.clip(values, min=-most, max=most).astype(dtype)


def setup_inputs(seed: int = 0) -> dict:
    arg_keys = jax.random.split(jax.random.key(seed), 12)
    atom_state = draw_atom_state(jax.random.fold_in(arg_keys[11], 71), 0)
    atom_token = jnp.searchsorted(jnp.cumsum(ragged_sizes(arg_keys[1], TOKENS, ATOMS, 24, 0)), jnp.arange(ATOMS), side="right").astype(jnp.int32)
    window_valid = with_ends(jax.random.randint(arg_keys[2], (WINDOWS,), 1, QWIN + 1), jax.random.fold_in(arg_keys[2], 1), 1, QWIN).astype(jnp.int32)
    attend_gain = jnp.clip(1.0 + 0.15 * jax.random.normal(arg_keys[3], (WIDTH,), jnp.float32), 0.25, 1.75)
    project_weight = draw_project_weight(jax.random.fold_in(arg_keys[11], 71), 0)
    output_weight = bell_draw(arg_keys[5], (WIDTH, WIDTH), (WIDTH // 8) ** -0.5, 1.5)
    token_bias = jnp.clip(jax.random.uniform(arg_keys[6], (HEADS,), jnp.float32, -2.0, 2.0), -2.0, 2.0)
    transit_gain = jnp.clip(1.0 + 0.15 * jax.random.normal(arg_keys[7], (WIDTH,), jnp.float32), 0.25, 1.75)
    transit_weight = bell_draw(arg_keys[8], (WIDTH, 2 * TRANS), WIDTH ** -0.5, 0.5)
    return_weight = bell_draw(arg_keys[9], (TRANS, WIDTH), TRANS ** -0.5, 0.375)
    cotangent = bell_draw(arg_keys[10], (SAMPLES, ATOMS, WIDTH), 1.0, 6.0, ((0, 4), (1, 8)))
    return {"atom_state": atom_state, "atom_token": atom_token, "window_valid": window_valid, "attend_gain": attend_gain, "project_weight": project_weight, "output_weight": output_weight, "token_bias": token_bias, "transit_gain": transit_gain, "transit_weight": transit_weight, "return_weight": return_weight, "cotangent": cotangent}


PRECISE = lax.Precision.HIGHEST
EPSILON = 1e-05
CLIP_NORM = 256.0

def normalize(values, scaling):
    values = values.astype(jnp.float32)
    center = lax.optimization_barrier(jnp.mean(values, axis=-1, keepdims=True))
    shifted = values - center
    variance = lax.optimization_barrier(jnp.mean(shifted * shifted, axis=-1, keepdims=True))
    return shifted * lax.rsqrt(variance + EPSILON) * scaling

def token_codes(atom_token, window_valid):
    windows_here = window_valid.shape[0]
    slots = lax.broadcasted_iota(jnp.int32, (windows_here, QWIN), 1)
    inside = (slots < window_valid[:, None]).reshape(-1)
    return jnp.where(inside, atom_token + 1, 0).astype(jnp.int32)

def attend(queries, pairs, query_ids, ext_ids, token_bias):
    channels = queries.shape[1]
    window_count = queries.shape[0] // QWIN
    extra_blocks = 2 * HALO // QWIN
    span_blocks = KWIN // QWIN
    head_dim = channels // HEADS
    blocks = pairs.reshape(window_count + extra_blocks, QWIN, 2 * channels)
    gathered = jnp.concatenate([blocks[offset:offset + window_count] for offset in range(span_blocks)], axis=1)
    code_blocks = ext_ids.reshape(window_count + extra_blocks, QWIN)
    key_ids = jnp.concatenate([code_blocks[offset:offset + window_count] for offset in range(span_blocks)], axis=1)
    query_blocks = queries.reshape(window_count, QWIN, HEADS, head_dim)
    keys_in = gathered[:, :, :channels].reshape(window_count, KWIN, HEADS, head_dim)
    values_in = gathered[:, :, channels:].reshape(window_count, KWIN, HEADS, head_dim)
    scores = jnp.einsum('wqhd,wkhd->whqk', query_blocks, keys_in, precision=PRECISE) / jnp.sqrt(float(head_dim))
    query_codes = query_ids.reshape(window_count, QWIN)
    same_token = (query_codes[:, :, None] == key_ids[:, None, :]).astype(jnp.float32)
    scores = scores + token_bias[None, :, None, None] * same_token[:, None, :, :]
    usable_key = (key_ids > 0)[:, None, None, :]
    scores = jnp.where(usable_key, scores, -1e+30)
    highest = lax.stop_gradient(lax.optimization_barrier(jnp.max(scores, axis=-1, keepdims=True)))
    weights = jnp.exp(scores - highest)
    weights = weights / lax.optimization_barrier(jnp.sum(weights, axis=-1, keepdims=True))
    outcome = jnp.einsum('whqk,wkhd->wqhd', weights, values_in, precision=PRECISE)
    return outcome.reshape(window_count * QWIN, channels)

def reference(atom_state, atom_token, window_valid, attend_gain, project_weight, output_weight, token_bias, transit_gain, transit_weight, return_weight, cotangent):
    query_ids = token_codes(atom_token, window_valid)
    ext_ids = jnp.pad(query_ids, (HALO, HALO))
    channels = atom_state.shape[2]
    atom_total = atom_state.shape[1]

    def one_sample(carry, operands):
        state_rows, cot_rows = operands
        normed = normalize(state_rows, attend_gain).astype(jnp.bfloat16)
        projected = jnp.dot(normed, project_weight, preferred_element_type=jnp.float32).astype(jnp.bfloat16)
        queries = projected[:, :channels]
        pairs = jnp.pad(projected[:, channels:], ((HALO, HALO), (0, 0)))

        def local_attend(query_in, pairs_in, bias_in):
            return attend(query_in, pairs_in, query_ids, ext_ids, bias_in)
        outcome, pull_attend = jax.vjp(local_attend, queries.astype(jnp.float32), pairs.astype(jnp.float32), token_bias)
        attended = outcome.astype(jnp.bfloat16)
        residual = (state_rows.astype(jnp.float32) + jnp.dot(attended, output_weight, preferred_element_type=jnp.float32)).astype(jnp.bfloat16)
        transit_in = normalize(residual, transit_gain).astype(jnp.bfloat16)
        both_parts = jnp.dot(transit_in, transit_weight, preferred_element_type=jnp.float32)
        gate_part = both_parts[:, :TRANS]
        up_part = both_parts[:, TRANS:]
        gated = (jax.nn.silu(gate_part) * up_part).astype(jnp.bfloat16)
        block_rows = (residual.astype(jnp.float32) + jnp.dot(gated, return_weight, preferred_element_type=jnp.float32)).astype(jnp.bfloat16)
        grad_return = jnp.dot(gated.T, cot_rows, preferred_element_type=jnp.float32)
        back_gated = jnp.dot(cot_rows, return_weight.T, preferred_element_type=jnp.float32)
        sigmoid_gate = jax.nn.sigmoid(gate_part)
        back_gate = back_gated * up_part * sigmoid_gate * (1.0 + gate_part * (1.0 - sigmoid_gate))
        back_up = back_gated * gate_part * sigmoid_gate
        back_hidden = jnp.concatenate([back_gate, back_up], axis=1).astype(jnp.bfloat16)
        grad_transit = jnp.dot(transit_in.T, back_hidden, preferred_element_type=jnp.float32)
        back_transit = jnp.dot(back_hidden, transit_weight.T, preferred_element_type=jnp.float32)
        _, pull_second = jax.vjp(normalize, residual.astype(jnp.float32), transit_gain)
        back_res_norm, grad_transit_gain = pull_second(back_transit)
        back_residual = cot_rows.astype(jnp.float32) + back_res_norm
        back_res16 = back_residual.astype(jnp.bfloat16)
        grad_output = jnp.dot(attended.T, back_res16, preferred_element_type=jnp.float32)
        back_attended = jnp.dot(back_res16, output_weight.T, preferred_element_type=jnp.float32)
        back_queries, back_pairs, grad_bias = pull_attend(back_attended)
        back_projected = jnp.concatenate([back_queries, back_pairs[HALO:HALO + atom_total]], axis=1)
        grad_project = jnp.dot(normed.astype(jnp.float32).T, back_projected, precision=PRECISE)
        back_normed = jnp.dot(back_projected, project_weight.astype(jnp.float32).T, precision=PRECISE)
        _, pull_first = jax.vjp(normalize, state_rows.astype(jnp.float32), attend_gain)
        back_state_norm, grad_attend_gain = pull_first(back_normed)
        state_rows_grad = (back_residual + back_state_norm).astype(jnp.bfloat16)
        terms = (grad_attend_gain, grad_project, grad_output, grad_bias, grad_transit_gain, grad_transit, grad_return)
        carry = tuple((total + member for total, member in zip(carry, terms)))
        return (carry, (block_rows, state_rows_grad))
    start = (jnp.zeros((channels,), jnp.float32), jnp.zeros((channels, 3 * channels), jnp.float32), jnp.zeros((channels, channels), jnp.float32), jnp.zeros((HEADS,), jnp.float32), jnp.zeros((channels,), jnp.float32), jnp.zeros((channels, 2 * TRANS), jnp.float32), jnp.zeros((TRANS, channels), jnp.float32))
    totals, (block_out, state_grad) = lax.scan(one_sample, start, (atom_state, cotangent))
    squares = sum((jnp.sum(member * member) for member in totals))
    factor = CLIP_NORM / jnp.sqrt(squares + CLIP_NORM * CLIP_NORM)
    clipped = tuple((member * factor for member in totals))
    return (block_out, state_grad, clipped[0], clipped[1], clipped[2], clipped[3], clipped[4], clipped[5], clipped[6])
```

```python
import functools

import jax
import jax.numpy as jnp
from jax import lax
from jax.experimental import pallas as pl
from jax.experimental.pallas import tpu as pltpu
from jax.sharding import PartitionSpec as P

HEADS = 4
TRANS = 256
QWIN = 32
KWIN = 128
HALO = 48
EPSILON = 1e-05
CLIP_NORM = 256.0
BF = jnp.bfloat16
F32 = jnp.float32
LANES = 128
MESH = pl.DeviceIdType.MESH


def dot(a, b, dims=((1,), (0,))):
    return lax.dot_general(a, b, (dims, ((), ())), preferred_element_type=F32)


def dot_nt(a, b):
    return dot(a, b, ((1,), (1,)))


def dot_tn(a, b):
    return dot(a, b, ((0,), (0,)))


def stats(x):
    center = jnp.mean(x, axis=-1, keepdims=True)
    shifted = x - center
    rstd = lax.rsqrt(jnp.mean(shifted * shifted, axis=-1, keepdims=True) + EPSILON)
    return shifted * rstd, rstd


def norm_back(back, xhat, rstd, gain):
    scaled = back * gain
    first = jnp.mean(scaled, axis=-1, keepdims=True)
    second = jnp.mean(scaled * xhat, axis=-1, keepdims=True)
    return rstd * (scaled - first - xhat * second)


def split_hi_lo(row):
    hi = row.astype(BF)
    return hi, (row - hi.astype(F32)).astype(BF)


def local_kernel(
    ext_ref, cot_ref, kid_ref, qid_ref, again_ref, wp_ref, wo_ref, bias_ref, tgain_ref, wt_ref, wr_ref,
    out_ref, bnorm_ref, bres_ref, halo_ref, g_ref,
    normed_ref, q_ref, kv_ref, p_ref, att_ref, batt_ref, bq_ref, bkv_ref, mask_ref, same_ref, acc_ref, row_ref,
):
    samples, atoms, width = cot_ref.shape
    windows = atoms // QWIN
    hd = width // HEADS
    scale = 1.0 / (float(hd) ** 0.5)
    rows_h = lax.broadcasted_iota(jnp.int32, (HEADS * QWIN, width), 0) // QWIN
    cols_h = lax.broadcasted_iota(jnp.int32, (HEADS * QWIN, width), 1) // hd
    head_f = (rows_h == cols_h).astype(F32)
    head_b = head_f.astype(BF)
    again = again_ref[...]
    tgain = tgain_ref[...]

    acc_ref[...] = jnp.zeros_like(acc_ref)
    row_ref[...] = jnp.zeros_like(row_ref)
    bkv_ref[...] = jnp.zeros_like(bkv_ref)

    def masks(w, _):
        base = pl.multiple_of(w * QWIN, QWIN)
        kid = kid_ref[pl.ds(base, KWIN), :]
        same = (kid == qid_ref[pl.ds(w, 1), :]).astype(F32)
        same_ref[w] = same
        mask_ref[w] = jnp.where(kid > 0, same * bias_ref[...], -1e30)
        return 0

    lax.fori_loop(0, windows, masks, 0)

    def project(s, _):
        xhat, _r = stats(ext_ref[s].astype(F32))
        normed = (xhat * again).astype(BF)
        normed_ref[s] = normed
        both = dot(normed, wp_ref[...]).astype(BF)
        q_ref[s] = both[HALO : HALO + atoms, :width]
        kv_ref[s] = both[:, width:]
        return 0

    lax.fori_loop(0, samples, project, 0)

    def spread(rows):
        return jnp.concatenate([rows] * HEADS, axis=0) * head_b

    def gather_heads(value):
        return jnp.sum((value * head_f).reshape(HEADS, QWIN, width), axis=0)

    def attend(w, _):
        base = pl.multiple_of(w * QWIN, QWIN)
        mask = mask_ref[w]
        for s in range(samples):
            keys = kv_ref[s, pl.ds(base, KWIN), :width]
            vals = kv_ref[s, pl.ds(base, KWIN), width:]
            score = dot_nt(keys, spread(q_ref[s, pl.ds(base, QWIN), :])) * scale + mask
            weight = jnp.exp(score - jnp.max(score, axis=0, keepdims=True))
            prob = (weight * (1.0 / jnp.sum(weight, axis=0, keepdims=True))).astype(BF)
            p_ref[s, w] = prob
            att_ref[s, pl.ds(base, QWIN), :] = gather_heads(dot_tn(prob, vals)).astype(BF)
        return 0

    lax.fori_loop(0, windows, attend, 0)

    def transit(s, _):
        state = ext_ref[s, HALO : HALO + atoms, :].astype(F32)
        att = att_ref[s]
        residual = (state + dot(att, wo_ref[...])).astype(BF).astype(F32)
        xhat, rstd = stats(residual)
        tin = (xhat * tgain).astype(BF)
        both = dot(tin, wt_ref[...])
        gate, up = both[:, :TRANS], both[:, TRANS:]
        sig = 1.0 / (1.0 + jnp.exp(-gate))
        silu = gate * sig
        gated = (silu * up).astype(BF)
        out_ref[s] = (residual + dot(gated, wr_ref[...])).astype(BF)
        cot = cot_ref[s]
        acc_ref[8:10] += dot_tn(gated, cot).reshape(2, LANES, LANES)
        bg = dot_nt(cot, wr_ref[...])
        back_gate = (bg * up * sig * (1.0 + gate * (1.0 - sig))).astype(BF)
        back_up = (bg * silu).astype(BF)
        bh = jnp.concatenate([back_gate, back_up], axis=1)
        gt = dot_tn(tin, bh)
        for j in range(4):
            acc_ref[4 + j] += gt[:, j * LANES : (j + 1) * LANES]
        bt = dot_nt(bh, wt_ref[...])
        row_ref[1:2] += jnp.sum(bt * xhat, axis=0, keepdims=True)
        bres = cot.astype(F32) + norm_back(bt, xhat, rstd, tgain)
        bres_ref[s] = bres
        b16 = bres.astype(BF)
        acc_ref[3] += dot_tn(att, b16)
        batt_ref[s] = dot_nt(b16, wo_ref[...]).astype(BF)
        return 0

    lax.fori_loop(0, samples, transit, 0)

    def attend_back(w, _):
        base = pl.multiple_of(w * QWIN, QWIN)
        total = jnp.zeros((KWIN, LANES), F32)
        for s in range(samples):
            keys = kv_ref[s, pl.ds(base, KWIN), :width]
            vals = kv_ref[s, pl.ds(base, KWIN), width:]
            qs = spread(q_ref[s, pl.ds(base, QWIN), :])
            bo = spread(batt_ref[s, pl.ds(base, QWIN), :])
            prob = p_ref[s, w]
            pf = prob.astype(F32)
            bp = dot_nt(vals, bo)
            pbp = pf * bp
            bs = pbp - pf * jnp.sum(pbp, axis=0, keepdims=True)
            total = total + bs
            b16 = (bs * scale).astype(BF)
            bq_ref[s, pl.ds(base, QWIN), :] = gather_heads(dot_tn(b16, keys)).astype(BF)
            bkv_ref[s, pl.ds(base, KWIN), :width] += dot(b16, qs)
            bkv_ref[s, pl.ds(base, KWIN), width:] += dot(prob, bo)
        row_ref[2:3] += jnp.sum(total * same_ref[w], axis=0, keepdims=True)
        return 0

    lax.fori_loop(0, windows, attend_back, 0)

    def finish(s, _):
        normed = normed_ref[s]
        bkv = bkv_ref[s].astype(BF)
        bq = bq_ref[s]
        acc_ref[0] += dot_tn(normed[HALO : HALO + atoms], bq)
        gkv = dot_tn(normed, bkv)
        acc_ref[1] += gkv[:, :LANES]
        acc_ref[2] += gkv[:, LANES:]
        back = dot_nt(bkv, wp_ref[:, width:])
        own = back[HALO : HALO + atoms] + dot_nt(bq, wp_ref[:, :width])
        xhat, _r = stats(ext_ref[s].astype(F32))
        halo_before = back[:HALO]
        halo_after = back[HALO + atoms :]
        row_ref[0:1] += (
            jnp.sum(own * xhat[HALO : HALO + atoms], axis=0, keepdims=True)
            + jnp.sum(halo_before * xhat[:HALO], axis=0, keepdims=True)
            + jnp.sum(halo_after * xhat[HALO + atoms :], axis=0, keepdims=True)
        )
        halo_ref[0, s] = halo_after.astype(BF)
        halo_ref[1, s] = halo_before.astype(BF)
        bnorm_ref[s] = own
        return 0

    lax.fori_loop(0, samples, finish, 0)

    blocks = acc_ref.shape[0]
    g_ref[: blocks * LANES, :] = acc_ref[...].reshape(blocks * LANES, LANES).astype(BF)
    rest = g_ref.shape[0] - blocks * LANES
    pieces = []
    for i in range(3):
        hi, lo = split_hi_lo(row_ref[i : i + 1])
        pieces += [hi.astype(F32), lo.astype(F32)]
    pieces.append(jnp.zeros((rest - 6, LANES), F32))
    g_ref[blocks * LANES :, :] = jnp.concatenate(pieces, axis=0).astype(BF)


def reduce_kernel(
    A, S,
    g_ref, halo_ref, bnorm_ref, bres_ref, state_ref, again_ref,
    sg_ref, gag_ref, gp_ref, go_ref, gb_ref, gtg_ref, gt_ref, gr_ref,
    recv1, send2, recv2, gath, rim,
    s1, r1, s2, r2, s3, r3, s4, r4, sh, rh,
):
    me_s, me_a = lax.axis_index("samp"), lax.axis_index("atom")
    samples, atoms, width = state_ref.shape

    barrier = pltpu.get_barrier_semaphore()
    for d in range(1, A):
        pl.semaphore_signal(barrier, inc=1, device_id=(me_s, lax.rem(me_a + d, A)), device_id_type=MESH)
    for d in range(1, S):
        pl.semaphore_signal(barrier, inc=1, device_id=(lax.rem(me_s + d, S), me_a), device_id_type=MESH)
    pl.semaphore_wait(barrier, A + S - 2)

    def remote(src, dst, ss, rs, dev):
        return pltpu.make_async_remote_copy(
            src_ref=src, dst_ref=dst, send_sem=ss, recv_sem=rs, device_id=dev, device_id_type=MESH
        )

    first = []
    for d in range(1, A):
        peer = lax.rem(me_a + d, A)
        copy = remote(g_ref.at[peer], recv1.at[d - 1], s1.at[d - 1], r1.at[d - 1], (me_s, peer))
        copy.start()
        first.append(copy)

    up = remote(halo_ref.at[0], rim.at[0], sh.at[0], rh.at[0], (me_s, lax.rem(me_a + 1, A)))
    down = remote(halo_ref.at[1], rim.at[1], sh.at[1], rh.at[1], (me_s, lax.rem(me_a + A - 1, A)))
    up.start()
    down.start()

    total = g_ref[me_a].astype(F32)
    for d in range(1, A):
        first[d - 1].wait_recv()
        total = total + recv1[d - 1].astype(F32)
    send2[...] = total.astype(BF)

    second = []
    for d in range(1, S):
        peer = lax.rem(me_s + d, S)
        copy = remote(send2.at[peer], recv2.at[d - 1], s2.at[d - 1], r2.at[d - 1], (peer, me_a))
        copy.start()
        second.append(copy)

    up.wait()
    down.wait()
    has_before = (me_a > 0).astype(F32)
    has_after = (me_a < A - 1).astype(F32)
    again = again_ref[...]

    def one(s, _):
        xhat, rstd = stats(state_ref[s].astype(F32))
        own = bnorm_ref[s]
        head = own[:HALO] + rim[0, s].astype(F32) * has_before
        tail = own[atoms - HALO :] + rim[1, s].astype(F32) * has_after
        back = jnp.concatenate([head, own[HALO : atoms - HALO], tail], axis=0)
        sg_ref[s] = (bres_ref[s] + norm_back(back, xhat, rstd, again)).astype(BF)
        return 0

    mine = send2[me_s].astype(F32)
    for d in range(1, S):
        second[d - 1].wait_recv()
        mine = mine + recv2[d - 1].astype(F32)
    gath[me_a, me_s] = mine.astype(BF)

    third = []
    for d in range(1, S):
        peer = lax.rem(me_s + d, S)
        copy = remote(gath.at[me_a, me_s], gath.at[me_a, me_s], s3.at[d - 1], r3.at[d - 1], (peer, me_a))
        copy.start()
        third.append(copy)
    for d in range(1, S):
        src = lax.rem(me_s + S - d, S)
        remote(gath.at[me_a, src], gath.at[me_a, src], s3.at[d - 1], r3.at[d - 1], (src, me_a)).wait_recv()
    fourth = []
    for d in range(1, A):
        peer = lax.rem(me_a + d, A)
        copy = remote(gath.at[me_a], gath.at[me_a], s4.at[d - 1], r4.at[d - 1], (me_s, peer))
        copy.start()
        fourth.append(copy)

    lax.fori_loop(0, samples, one, 0)

    for d in range(1, A):
        src = lax.rem(me_a + A - d, A)
        remote(gath.at[src], gath.at[src], s4.at[d - 1], r4.at[d - 1], (me_s, src)).wait_recv()
    for copy in first + second + third + fourth:
        copy.wait_send()

    flat = gath[...].astype(F32).reshape(-1, LANES)
    blocks = [flat[j * LANES : (j + 1) * LANES] for j in range(10)]
    rest = flat[10 * LANES : 10 * LANES + 6]
    rows = [rest[0:1] + rest[1:2], rest[2:3] + rest[3:4], rest[4:5] + rest[5:6]]
    lane_head = lax.broadcasted_iota(jnp.int32, (1, LANES), 1)
    bias = jnp.zeros((1, LANES), F32)
    for h in range(HEADS):
        part = jnp.sum(jnp.where(lane_head // QWIN == h, rows[2], 0.0), axis=1, keepdims=True)
        bias = bias + jnp.where(lane_head == h, part, 0.0)
    sq = blocks[0] * blocks[0]
    for b in blocks[1:]:
        sq = sq + b * b
    sq = jnp.sum(sq, axis=0, keepdims=True) + rows[0] * rows[0] + rows[1] * rows[1] + bias * bias
    squares = jnp.sum(sq, axis=1, keepdims=True)
    factor = CLIP_NORM / jnp.sqrt(squares + CLIP_NORM * CLIP_NORM)
    gag_ref[...] = rows[0] * factor
    gtg_ref[...] = rows[1] * factor
    gb_ref[...] = bias * factor
    for j in range(3):
        gp_ref[:, j * LANES : (j + 1) * LANES] = blocks[j] * factor
    go_ref[...] = blocks[3] * factor
    for j in range(4):
        gt_ref[:, j * LANES : (j + 1) * LANES] = blocks[4 + j] * factor
    for j in range(2):
        gr_ref[j * LANES : (j + 1) * LANES, :] = blocks[8 + j] * factor


def on_device(A, S, atom_state, atom_token, window_valid, attend_gain, project_weight, output_weight,
              token_bias, transit_gain, transit_weight, return_weight, cotangent):
    samples, atoms, width = atom_state.shape
    windows = window_valid.shape[0]
    ext = atoms + 2 * HALO
    up_pairs = [(i, i + 1) for i in range(A - 1)]
    down_pairs = [(i + 1, i) for i in range(A - 1)]
    slots = lax.broadcasted_iota(jnp.int32, (windows, QWIN), 1)
    ids = jnp.where((slots < window_valid[:, None]).reshape(-1), atom_token + 1, 0)
    before = lax.ppermute(atom_state[:, atoms - HALO :], "atom", up_pairs)
    after = lax.ppermute(atom_state[:, :HALO], "atom", down_pairs)
    ids_before = lax.ppermute(ids[atoms - HALO :], "atom", up_pairs)
    ids_after = lax.ppermute(ids[:HALO], "atom", down_pairs)
    ext_state = jnp.concatenate([before, atom_state, after], axis=1)
    ext_ids = jnp.concatenate([ids_before, ids, ids_after])
    kid = jnp.broadcast_to(ext_ids[:, None], (ext, LANES))
    qid = jnp.tile(ids.reshape(windows, QWIN), (1, HEADS))
    again = attend_gain.reshape(1, width)
    tgain = transit_gain.reshape(1, width)
    bias_row = jnp.repeat(token_bias, QWIN).reshape(1, HEADS * QWIN)
    shards = A * S
    need = 10 * LANES + 6
    per = -(-need // (shards * 16)) * 16
    vm = pl.BlockSpec(memory_space=pltpu.VMEM)
    sds = jax.ShapeDtypeStruct
    act = (samples, atoms, width)
    block_out, bnorm, bres, halo, grads = pl.pallas_call(
        local_kernel,
        out_shape=(sds(act, BF), sds(act, F32), sds(act, F32), sds((2, samples, HALO, width), BF),
                   sds((shards * per, LANES), BF)),
        in_specs=[vm] * 11,
        out_specs=(vm,) * 5,
        scratch_shapes=[
            pltpu.VMEM((samples, ext, width), BF),
            pltpu.VMEM(act, BF),
            pltpu.VMEM((samples, ext, 2 * width), BF),
            pltpu.VMEM((samples, windows, KWIN, LANES), BF),
            pltpu.VMEM(act, BF),
            pltpu.VMEM(act, BF),
            pltpu.VMEM(act, BF),
            pltpu.VMEM((samples, ext, 2 * width), F32),
            pltpu.VMEM((windows, KWIN, LANES), F32),
            pltpu.VMEM((windows, KWIN, LANES), F32),
            pltpu.VMEM((10, LANES, LANES), F32),
            pltpu.VMEM((8, LANES), F32),
        ],
        name="local",
    )(ext_state, cotangent, kid, qid, again, project_weight, output_weight, bias_row, tgain,
      transit_weight, return_weight)
    grads = grads.reshape(A, S, per, LANES)
    dma = pltpu.SemaphoreType.DMA
    sg, gag, gp, go, gb, gtg, gt, gr = pl.pallas_call(
        functools.partial(reduce_kernel, A, S),
        out_shape=(sds(act, BF), sds((1, width), F32), sds((width, 3 * width), F32), sds((width, width), F32),
                   sds((1, LANES), F32), sds((1, width), F32), sds((width, 2 * TRANS), F32),
                   sds((TRANS, width), F32)),
        in_specs=[vm] * 6,
        out_specs=(vm,) * 8,
        scratch_shapes=[
            pltpu.VMEM((A - 1, S, per, LANES), BF),
            pltpu.VMEM((S, per, LANES), BF),
            pltpu.VMEM((S - 1, per, LANES), BF),
            pltpu.VMEM((A, S, per, LANES), BF),
            pltpu.VMEM((2, samples, HALO, width), BF),
            dma((A - 1,)), dma((A - 1,)), dma((S - 1,)), dma((S - 1,)), dma((S - 1,)), dma((S - 1,)),
            dma((A - 1,)), dma((A - 1,)), dma((2,)), dma((2,)),
        ],
        compiler_params=pltpu.CompilerParams(collective_id=0, has_side_effects=True),
        name="reduce",
    )(grads, halo, bnorm, bres, atom_state, again)
    return (block_out, sg, gag.reshape(width), gp, go, gb[0, :HEADS], gtg.reshape(width), gt, gr)


def solution(mesh):
    A, S = mesh.shape["atom"], mesh.shape["samp"]
    act = P("samp", "atom", None)
    return jax.shard_map(
        functools.partial(on_device, A, S),
        mesh=mesh,
        in_specs=(act, P("atom"), P("atom"), P(), P(), P(), P(), P(), P(), P(), act),
        out_specs=(act, act, P(), P(), P(), P(), P(), P(), P()),
        check_vma=False,
    )
```

```python
import functools

import jax
import jax.numpy as jnp
from jax import lax
from jax.experimental import pallas as pl
from jax.experimental.pallas import tpu as pltpu
from jax.sharding import PartitionSpec as P

HEADS = 4
TRANS = 256
QWIN = 32
KWIN = 128
HALO = 48
EPSILON = 1e-05
CLIP_NORM = 256.0
BF = jnp.bfloat16
F32 = jnp.float32
LANES = 128
MESH = pl.DeviceIdType.MESH


def dot(a, b, dims=((1,), (0,))):
    return lax.dot_general(a, b, (dims, ((), ())), preferred_element_type=F32)


def dot_nt(a, b):
    return dot(a, b, ((1,), (1,)))


def dot_tn(a, b):
    return dot(a, b, ((0,), (0,)))


def stats(x):
    center = jnp.mean(x, axis=-1, keepdims=True)
    shifted = x - center
    rstd = lax.rsqrt(jnp.mean(shifted * shifted, axis=-1, keepdims=True) + EPSILON)
    return shifted * rstd, rstd


def norm_back(back, xhat, rstd, gain):
    scaled = back * gain
    first = jnp.mean(scaled, axis=-1, keepdims=True)
    second = jnp.mean(scaled * xhat, axis=-1, keepdims=True)
    return rstd * (scaled - first - xhat * second)


def split_hi_lo(row):
    hi = row.astype(BF)
    return hi, (row - hi.astype(F32)).astype(BF)


def mega_kernel(
    A, S,
    state_ref, cot_ref, qid_ref, again_ref, wp_ref, wo_ref, tb_ref, tgain_ref, wt_ref, wr_ref,
    out_ref, sg_ref, ga_ref, gb_ref,
    edge_ref, eid_ref, kid_ref, normed_ref, q_ref, kv_ref, p_ref, att_ref, batt_ref, bq_ref, bkv_ref,
    mask_ref, same_ref, acc_ref, row_ref, bnorm_ref, bres_ref, halo_ref, rim_ref,
    send_a, mid_a, in1_a, in2_a, all_a, send_b, mid_b, in1_b, in2_b, all_b,
    esend, erecv, hsend, hrecv, sems_a, sems_b,
):
    me_s, me_a = lax.axis_index("samp"), lax.axis_index("atom")
    samples, atoms, width = cot_ref.shape
    windows = atoms // QWIN
    near = -(-HALO // QWIN)
    hd = width // HEADS
    scale = 1.0 / (float(hd) ** 0.5)
    right, left = lax.rem(me_a + 1, A), lax.rem(me_a + A - 1, A)

    barrier = pltpu.get_barrier_semaphore()
    for d in range(1, A):
        pl.semaphore_signal(barrier, inc=1, device_id=(me_s, lax.rem(me_a + d, A)), device_id_type=MESH)
    for d in range(1, S):
        pl.semaphore_signal(barrier, inc=1, device_id=(lax.rem(me_s + d, S), me_a), device_id_type=MESH)

    def remote(src, dst, ss, rs, dev):
        return pltpu.make_async_remote_copy(
            src_ref=src, dst_ref=dst, send_sem=ss, recv_sem=rs, device_id=dev, device_id_type=MESH
        )

    rows_h = lax.broadcasted_iota(jnp.int32, (HEADS * QWIN, width), 0) // QWIN
    cols_h = lax.broadcasted_iota(jnp.int32, (HEADS * QWIN, width), 1) // hd
    head_f = (rows_h == cols_h).astype(F32)
    head_b = head_f.astype(BF)
    again = again_ref[...]
    tgain = tgain_ref[...]
    lane_head = lax.broadcasted_iota(jnp.int32, (1, LANES), 1) // QWIN
    bias_row = jnp.zeros((1, LANES), F32)
    for h in range(HEADS):
        bias_row = jnp.where(lane_head == h, tb_ref[h], bias_row)

    acc_ref[...] = jnp.zeros_like(acc_ref)
    row_ref[...] = jnp.zeros_like(row_ref)
    bkv_ref[...] = jnp.zeros_like(bkv_ref)

    def project(s, _):
        xhat, _r = stats(state_ref[s].astype(F32))
        normed = (xhat * again).astype(BF)
        normed_ref[s, HALO : HALO + atoms] = normed
        both = dot(normed, wp_ref[...]).astype(BF)
        q_ref[s] = both[:, :width]
        kv_ref[s, HALO : HALO + atoms] = both[:, width:]
        return 0

    lax.fori_loop(0, samples, project, 0)

    pl.semaphore_wait(barrier, A + S - 2)
    edges = [
        remote(state_ref.at[:, pl.ds(atoms - HALO, HALO), :], edge_ref.at[0], esend.at[0], erecv.at[0], (me_s, right)),
        remote(state_ref.at[:, pl.ds(0, HALO), :], edge_ref.at[1], esend.at[1], erecv.at[1], (me_s, left)),
        remote(qid_ref.at[pl.ds(windows - near, near)], eid_ref.at[0], esend.at[2], erecv.at[2], (me_s, right)),
        remote(qid_ref.at[pl.ds(0, near)], eid_ref.at[1], esend.at[3], erecv.at[3], (me_s, left)),
    ]
    for copy in edges:
        copy.start()

    def columns(rows):
        count = rows.shape[0]
        full = jnp.concatenate([rows.astype(F32), jnp.zeros((LANES - count, LANES), F32)], axis=0)
        turned = full.T
        return [jnp.broadcast_to(turned[:QWIN, j : j + 1], (QWIN, LANES)) for j in range(count)]

    for j, column in enumerate(columns(qid_ref[:, 0, :])):
        kid_ref[HALO + j * QWIN : HALO + (j + 1) * QWIN, :] = column

    def masks(w):
        base = pl.multiple_of(w * QWIN, QWIN)
        kid = kid_ref[pl.ds(base, KWIN), :]
        same = (kid == qid_ref[w][0:1].astype(F32)).astype(F32)
        same_ref[w] = same
        mask = jnp.where(kid > 0.0, same * bias_row, -1e30)
        mask_ref[w] = mask
        return mask

    def spread(rows):
        return jnp.concatenate([rows] * HEADS, axis=0) * head_b

    def gather_heads(value):
        return jnp.sum((value * head_f).reshape(HEADS, QWIN, width), axis=0)

    def attend_at(w):
        base = pl.multiple_of(w * QWIN, QWIN)
        mask = masks(w)
        for s in range(samples):
            keys = kv_ref[s, pl.ds(base, KWIN), :width]
            vals = kv_ref[s, pl.ds(base, KWIN), width:]
            score = dot_nt(keys, spread(q_ref[s, pl.ds(base, QWIN), :])) * scale + mask
            weight = jnp.exp(score - jnp.max(score, axis=0, keepdims=True))
            prob = (weight * (1.0 / jnp.sum(weight, axis=0, keepdims=True))).astype(BF)
            p_ref[s, w] = prob
            att_ref[s, pl.ds(base, QWIN), :] = gather_heads(dot_tn(prob, vals)).astype(BF)

    def attend(w, _):
        attend_at(w)
        return 0

    lax.fori_loop(near, windows - near, attend, 0)

    for copy in edges:
        copy.wait()
    has_before = (me_a > 0).astype(F32)
    has_after = (me_a < A - 1).astype(F32)
    for side, has in ((0, has_before), (1, has_after)):
        cols = jnp.concatenate(columns(eid_ref[side, :, 0, :]), axis=0) * has
        if side == 0:
            kid_ref[:HALO, :] = cols[near * QWIN - HALO :]
        else:
            kid_ref[HALO + atoms :, :] = cols[:HALO]

    def project_edge(s, _):
        both_edges = jnp.concatenate([edge_ref[0, s], edge_ref[1, s]], axis=0)
        xhat, _r = stats(both_edges.astype(F32))
        normed = (xhat * again).astype(BF)
        normed_ref[s, :HALO] = normed[:HALO]
        normed_ref[s, HALO + atoms :] = normed[HALO:]
        both = dot(normed, wp_ref[:, width:]).astype(BF)
        kv_ref[s, :HALO] = both[:HALO]
        kv_ref[s, HALO + atoms :] = both[HALO:]
        return 0

    lax.fori_loop(0, samples, project_edge, 0)

    def attend_edge(i, _):
        attend_at(jnp.where(i < near, i, windows - 2 * near + i))
        return 0

    lax.fori_loop(0, 2 * near, attend_edge, 0)

    def transit(s, _):
        state = state_ref[s].astype(F32)
        att = att_ref[s]
        residual = (state + dot(att, wo_ref[...])).astype(BF).astype(F32)
        xhat, rstd = stats(residual)
        tin = (xhat * tgain).astype(BF)
        both = dot(tin, wt_ref[...])
        gate, up = both[:, :TRANS], both[:, TRANS:]
        sig = 1.0 / (1.0 + jnp.exp(-gate))
        silu = gate * sig
        gated = (silu * up).astype(BF)
        out_ref[s] = (residual + dot(gated, wr_ref[...])).astype(BF)
        cot = cot_ref[s]
        acc_ref[5:7] += dot_tn(gated, cot).reshape(2, LANES, LANES)
        bg = dot_nt(cot, wr_ref[...])
        back_gate = (bg * up * sig * (1.0 + gate * (1.0 - sig))).astype(BF)
        back_up = (bg * silu).astype(BF)
        bh = jnp.concatenate([back_gate, back_up], axis=1)
        gt = dot_tn(tin, bh)
        for j in range(4):
            acc_ref[1 + j] += gt[:, j * LANES : (j + 1) * LANES]
        bt = dot_nt(bh, wt_ref[...])
        row_ref[1:2] += jnp.sum(bt * xhat, axis=0, keepdims=True)
        bres = cot.astype(F32) + norm_back(bt, xhat, rstd, tgain)
        bres_ref[s] = bres
        b16 = bres.astype(BF)
        acc_ref[0] += dot_tn(att, b16)
        batt_ref[s] = dot_nt(b16, wo_ref[...]).astype(BF)
        return 0

    lax.fori_loop(0, samples, transit, 0)

    class Reduce:
        def __init__(self, send, in1, mid, in2, full, sems):
            self.send, self.in1, self.mid, self.in2, self.full, self.sems = send, in1, mid, in2, full, sems
            self.started = []

        def over_atom(self, src_of, dst_of, k):
            copies = []
            for d in range(1, A):
                peer = lax.rem(me_a + d, A)
                copy = remote(src_of(peer), dst_of(d), self.sems.at[k, 0, d - 1], self.sems.at[k, 1, d - 1], (me_s, peer))
                copy.start()
                copies.append(copy)
            self.started += copies
            return copies

        def over_samp(self, src_of, dst_of, k):
            copies = []
            for d in range(1, S):
                peer = lax.rem(me_s + d, S)
                copy = remote(src_of(peer), dst_of(d), self.sems.at[k, 0, d - 1], self.sems.at[k, 1, d - 1], (peer, me_a))
                copy.start()
                copies.append(copy)
            self.started += copies
            return copies

        def step1(self):
            self.c1 = self.over_atom(lambda p: self.send.at[p], lambda d: self.in1.at[d - 1], 0)

        def step2(self):
            total = self.send[me_a].astype(F32)
            for d in range(1, A):
                self.c1[d - 1].wait_recv()
                total = total + self.in1[d - 1].astype(F32)
            self.mid[...] = total.astype(BF)
            self.c2 = self.over_samp(lambda p: self.mid.at[p], lambda d: self.in2.at[d - 1], 1)

        def step3(self):
            mine = self.mid[me_s].astype(F32)
            for d in range(1, S):
                self.c2[d - 1].wait_recv()
                mine = mine + self.in2[d - 1].astype(F32)
            self.full[me_a, me_s] = mine.astype(BF)
            self.over_samp(lambda p: self.full.at[me_a, me_s], lambda d: self.full.at[me_a, me_s], 2)

        def step4(self):
            for d in range(1, S):
                src = lax.rem(me_s + S - d, S)
                ref = self.full.at[me_a, src]
                remote(ref, ref, self.sems.at[2, 0, d - 1], self.sems.at[2, 1, d - 1], (src, me_a)).wait_recv()
            self.over_atom(lambda p: self.full.at[me_a], lambda d: self.full.at[me_a], 3)

        def step5(self):
            for d in range(1, A):
                src = lax.rem(me_a + A - d, A)
                ref = self.full.at[src]
                remote(ref, ref, self.sems.at[3, 0, d - 1], self.sems.at[3, 1, d - 1], (me_s, src)).wait_recv()
            for copy in self.started:
                copy.wait_send()

    def pack(dst, parts):
        rows = A * S * dst.shape[2]
        used = sum(p.shape[0] for p in parts)
        if rows > used:
            parts = parts + [jnp.zeros((rows - used, LANES), F32)]
        dst[...] = jnp.concatenate(parts, axis=0).reshape(dst.shape).astype(BF)

    red_a = Reduce(send_a, in1_a, mid_a, in2_a, all_a, sems_a)
    red_b = Reduce(send_b, in1_b, mid_b, in2_b, all_b, sems_b)

    pack(send_a, [acc_ref[j] for j in range(7)])
    red_a.step1()

    def attend_back(w, _):
        base = pl.multiple_of(w * QWIN, QWIN)
        total = jnp.zeros((KWIN, LANES), F32)
        for s in range(samples):
            keys = kv_ref[s, pl.ds(base, KWIN), :width]
            vals = kv_ref[s, pl.ds(base, KWIN), width:]
            qs = spread(q_ref[s, pl.ds(base, QWIN), :])
            bo = spread(batt_ref[s, pl.ds(base, QWIN), :])
            prob = p_ref[s, w]
            pf = prob.astype(F32)
            bp = dot_nt(vals, bo)
            pbp = pf * bp
            bs = pbp - pf * jnp.sum(pbp, axis=0, keepdims=True)
            total = total + bs
            b16 = (bs * scale).astype(BF)
            bq_ref[s, pl.ds(base, QWIN), :] = gather_heads(dot_tn(b16, keys)).astype(BF)
            bkv_ref[s, pl.ds(base, KWIN), :width] += dot(b16, qs)
            bkv_ref[s, pl.ds(base, KWIN), width:] += dot(prob, bo)
        row_ref[2:3] += jnp.sum(total * same_ref[w], axis=0, keepdims=True)
        return 0

    half = windows // 2
    lax.fori_loop(0, half, attend_back, 0)
    red_a.step2()
    lax.fori_loop(half, windows, attend_back, 0)
    red_a.step3()

    def finish(s, _):
        normed = normed_ref[s]
        bkv = bkv_ref[s].astype(BF)
        bq = bq_ref[s]
        acc_ref[7] += dot_tn(normed[HALO : HALO + atoms], bq)
        gkv = dot_tn(normed, bkv)
        acc_ref[8] += gkv[:, :LANES]
        acc_ref[9] += gkv[:, LANES:]
        back = dot_nt(bkv, wp_ref[:, width:])
        own = back[HALO : HALO + atoms] + dot_nt(bq, wp_ref[:, :width])
        xhat, _r = stats(state_ref[s].astype(F32))
        xb, _r = stats(edge_ref[0, s].astype(F32))
        xa, _r = stats(edge_ref[1, s].astype(F32))
        halo_before = back[:HALO]
        halo_after = back[HALO + atoms :]
        row_ref[0:1] += (
            jnp.sum(own * xhat, axis=0, keepdims=True)
            + jnp.sum(halo_before * xb, axis=0, keepdims=True)
            + jnp.sum(halo_after * xa, axis=0, keepdims=True)
        )
        halo_ref[0, s] = halo_after.astype(BF)
        halo_ref[1, s] = halo_before.astype(BF)
        bnorm_ref[s] = own
        return 0

    lax.fori_loop(0, samples, finish, 0)

    pieces = [acc_ref[7 + j] for j in range(3)]
    for i in range(3):
        hi, lo = split_hi_lo(row_ref[i : i + 1])
        pieces += [hi.astype(F32), lo.astype(F32)]
    pieces[3:] = [jnp.concatenate(pieces[3:] + [jnp.zeros((10, LANES), F32)], axis=0)]
    pack(send_b, pieces)
    red_b.step1()
    rims = [
        remote(halo_ref.at[0], rim_ref.at[0], hsend.at[0], hrecv.at[0], (me_s, right)),
        remote(halo_ref.at[1], rim_ref.at[1], hsend.at[1], hrecv.at[1], (me_s, left)),
    ]
    for copy in rims:
        copy.start()
    red_a.step4()
    red_b.step2()
    for copy in rims:
        copy.wait()

    def close(s, _):
        xhat, rstd = stats(state_ref[s].astype(F32))
        own = bnorm_ref[s]
        top = own[:HALO] + rim_ref[0, s].astype(F32) * has_before
        bottom = own[atoms - HALO :] + rim_ref[1, s].astype(F32) * has_after
        back = jnp.concatenate([top, own[HALO : atoms - HALO], bottom], axis=0)
        sg_ref[s] = (bres_ref[s] + norm_back(back, xhat, rstd, again)).astype(BF)
        return 0

    lax.fori_loop(0, samples // 2, close, 0)
    red_b.step3()
    lax.fori_loop(samples // 2, samples, close, 0)
    red_b.step4()
    red_a.step5()
    ga_ref[...] = all_a[...]
    red_b.step5()
    gb_ref[...] = all_b[...]


def clip_kernel(ga_ref, gb_ref, out_in, sg_in, out_ref, sg_ref, gag_ref, gp_ref, go_ref, gb_out, gtg_ref, gt_ref, gr_ref):
    out_ref[...] = out_in[...]
    sg_ref[...] = sg_in[...]
    fa = ga_ref[...].astype(F32).reshape(-1, LANES)
    fb = gb_ref[...].astype(F32).reshape(-1, LANES)
    blocks = [fa[j * LANES : (j + 1) * LANES] for j in range(7)] + [fb[j * LANES : (j + 1) * LANES] for j in range(3)]
    rest = fb[3 * LANES : 3 * LANES + 6]
    rows = [rest[0:1] + rest[1:2], rest[2:3] + rest[3:4], rest[4:5] + rest[5:6]]
    lane = lax.broadcasted_iota(jnp.int32, (1, LANES), 1)
    bias = jnp.zeros((1, LANES), F32)
    for h in range(HEADS):
        part = jnp.sum(jnp.where(lane // QWIN == h, rows[2], 0.0), axis=1, keepdims=True)
        bias = bias + jnp.where(lane == h, part, 0.0)
    sq = blocks[0] * blocks[0]
    for b in blocks[1:]:
        sq = sq + b * b
    sq = jnp.sum(sq, axis=0, keepdims=True) + rows[0] * rows[0] + rows[1] * rows[1] + bias * bias
    squares = jnp.sum(sq, axis=1, keepdims=True)
    factor = CLIP_NORM / jnp.sqrt(squares + CLIP_NORM * CLIP_NORM)
    gag_ref[...] = rows[0] * factor
    gtg_ref[...] = rows[1] * factor
    gb_out[...] = bias * factor
    go_ref[...] = blocks[0] * factor
    for j in range(4):
        gt_ref[:, j * LANES : (j + 1) * LANES] = blocks[1 + j] * factor
    for j in range(2):
        gr_ref[j * LANES : (j + 1) * LANES, :] = blocks[5 + j] * factor
    for j in range(3):
        gp_ref[:, j * LANES : (j + 1) * LANES] = blocks[7 + j] * factor


def on_device(A, S, atom_state, atom_token, window_valid, attend_gain, project_weight, output_weight,
              token_bias, transit_gain, transit_weight, return_weight, cotangent):
    samples, atoms, width = atom_state.shape
    windows = window_valid.shape[0]
    ext = atoms + 2 * HALO
    near = -(-HALO // QWIN)
    slots = lax.broadcasted_iota(jnp.int32, (windows, QWIN), 1)
    ids = jnp.where(slots < window_valid[:, None], atom_token.reshape(windows, QWIN) + 1, 0)
    qid = jnp.broadcast_to(jnp.tile(ids, (1, HEADS))[:, None, :], (windows, 8, LANES))
    again = attend_gain.reshape(1, width)
    tgain = transit_gain.reshape(1, width)
    shards = A * S
    per_a = -(-7 * LANES // (shards * 16)) * 16
    per_b = -(-(3 * LANES + 16) // (shards * 16)) * 16
    vm = pl.BlockSpec(memory_space=pltpu.VMEM)
    sds = jax.ShapeDtypeStruct
    act = (samples, atoms, width)
    dma = pltpu.SemaphoreType.DMA
    top = max(A, S) - 1

    def buffers(per):
        return [
            pltpu.VMEM((A, S, per, LANES), BF),
            pltpu.VMEM((S, per, LANES), BF),
            pltpu.VMEM((A - 1, S, per, LANES), BF),
            pltpu.VMEM((S - 1, per, LANES), BF),
            pltpu.VMEM((A, S, per, LANES), BF),
        ]

    block_out, sg, ga, gb = pl.pallas_call(
        functools.partial(mega_kernel, A, S),
        out_shape=(sds(act, BF), sds(act, BF), sds((A, S, per_a, LANES), BF), sds((A, S, per_b, LANES), BF)),
        in_specs=[vm] * 6 + [pl.BlockSpec(memory_space=pltpu.SMEM)] + [vm] * 3,
        out_specs=(vm,) * 4,
        scratch_shapes=[
            pltpu.VMEM((2, samples, HALO, width), BF),
            pltpu.VMEM((2, near, 8, LANES), jnp.int32),
            pltpu.VMEM((ext, LANES), F32),
            pltpu.VMEM((samples, ext, width), BF),
            pltpu.VMEM(act, BF),
            pltpu.VMEM((samples, ext, 2 * width), BF),
            pltpu.VMEM((samples, windows, KWIN, LANES), BF),
            pltpu.VMEM(act, BF),
            pltpu.VMEM(act, BF),
            pltpu.VMEM(act, BF),
            pltpu.VMEM((samples, ext, 2 * width), F32),
            pltpu.VMEM((windows, KWIN, LANES), F32),
            pltpu.VMEM((windows, KWIN, LANES), F32),
            pltpu.VMEM((10, LANES, LANES), F32),
            pltpu.VMEM((8, LANES), F32),
            pltpu.VMEM(act, F32),
            pltpu.VMEM(act, F32),
            pltpu.VMEM((2, samples, HALO, width), BF),
            pltpu.VMEM((2, samples, HALO, width), BF),
        ]
        + buffers(per_a)
        + buffers(per_b)
        + [dma((4,)), dma((4,)), dma((2,)), dma((2,)), dma((4, 2, top)), dma((4, 2, top))],
        compiler_params=pltpu.CompilerParams(collective_id=0, has_side_effects=True),
        name="block",
    )(atom_state, cotangent, qid, again, project_weight, output_weight, token_bias, tgain,
      transit_weight, return_weight)
    block_out, sg, gag, gp, go, gbias, gtg, gt, gr = pl.pallas_call(
        clip_kernel,
        out_shape=(sds(act, BF), sds(act, BF), sds((1, width), F32), sds((width, 3 * width), F32),
                   sds((width, width), F32), sds((1, LANES), F32), sds((1, width), F32),
                   sds((width, 2 * TRANS), F32), sds((TRANS, width), F32)),
        in_specs=[vm] * 4,
        out_specs=(vm,) * 9,
        name="clip",
    )(ga, gb, block_out, sg)
    return (block_out, sg, gag.reshape(width), gp, go, gbias[0, :HEADS], gtg.reshape(width), gt, gr)


def solution(mesh):
    A, S = mesh.shape["atom"], mesh.shape["samp"]
    act = P("samp", "atom", None)
    return jax.shard_map(
        functools.partial(on_device, A, S),
        mesh=mesh,
        in_specs=(act, P("atom"), P("atom"), P(), P(), P(), P(), P(), P(), P(), act),
        out_specs=(act, act, P(), P(), P(), P(), P(), P(), P()),
        check_vma=False,
    )
```

```python
import functools

import jax
import jax.numpy as jnp
from jax import lax
from jax.experimental import pallas as pl
from jax.experimental.pallas import tpu as pltpu
from jax.sharding import PartitionSpec as P

HEADS = 4
TRANS = 256
QWIN = 32
KWIN = 128
HALO = 48
EPSILON = 1e-05
CLIP_NORM = 256.0
BF = jnp.bfloat16
F32 = jnp.float32
LANES = 128
MESH = pl.DeviceIdType.MESH


def dot(a, b, dims=((1,), (0,))):
    return lax.dot_general(a, b, (dims, ((), ())), preferred_element_type=F32)


def dot_nt(a, b):
    return dot(a, b, ((1,), (1,)))


def dot_tn(a, b):
    return dot(a, b, ((0,), (0,)))


def stats(x):
    center = jnp.mean(x, axis=-1, keepdims=True)
    shifted = x - center
    rstd = lax.rsqrt(jnp.mean(shifted * shifted, axis=-1, keepdims=True) + EPSILON)
    return shifted * rstd, rstd


def norm_back(back, xhat, rstd, gain):
    scaled = back * gain
    first = jnp.mean(scaled, axis=-1, keepdims=True)
    second = jnp.mean(scaled * xhat, axis=-1, keepdims=True)
    return rstd * (scaled - first - xhat * second)


def split_hi_lo(row):
    hi = row.astype(BF)
    return hi, (row - hi.astype(F32)).astype(BF)


def mega_kernel(
    A, S,
    state_ref, cot_ref, qid_ref, again_ref, wp_ref, wo_ref, tb_ref, tgain_ref, wt_ref, wr_ref,
    out_ref, sg_ref, ga_ref, gb_ref,
    edge_ref, eid_ref, kid_ref, normed_ref, q_ref, kv_ref, p_ref, att_ref, batt_ref, bq_ref, bkv_ref,
    mask_ref, same_ref, acc_ref, row_ref, bnorm_ref, bres_ref, halo_ref, rim_ref,
    send_a, mid_a, in1_a, in2_a, all_a, send_b, mid_b, in1_b, in2_b, all_b,
    esend, erecv, hsend, hrecv, sems_a, sems_b, turn_ref,
):
    me_s, me_a = lax.axis_index("samp"), lax.axis_index("atom")
    samples, atoms, width = cot_ref.shape
    windows = atoms // QWIN
    near = -(-HALO // QWIN)
    hd = width // HEADS
    scale = 1.0 / (float(hd) ** 0.5)
    right, left = lax.rem(me_a + 1, A), lax.rem(me_a + A - 1, A)

    barrier = pltpu.get_barrier_semaphore()
    for d in range(1, A):
        pl.semaphore_signal(barrier, inc=1, device_id=(me_s, lax.rem(me_a + d, A)), device_id_type=MESH)
    for d in range(1, S):
        pl.semaphore_signal(barrier, inc=1, device_id=(lax.rem(me_s + d, S), me_a), device_id_type=MESH)

    def remote(src, dst, ss, rs, dev):
        return pltpu.make_async_remote_copy(
            src_ref=src, dst_ref=dst, send_sem=ss, recv_sem=rs, device_id=dev, device_id_type=MESH
        )

    rows_h = lax.broadcasted_iota(jnp.int32, (HEADS * QWIN, width), 0) // QWIN
    cols_h = lax.broadcasted_iota(jnp.int32, (HEADS * QWIN, width), 1) // hd
    head_f = (rows_h == cols_h).astype(F32)
    head_b = head_f.astype(BF)
    again = again_ref[...]
    tgain = tgain_ref[...]
    lane_head = lax.broadcasted_iota(jnp.int32, (1, LANES), 1) // QWIN
    bias_row = jnp.zeros((1, LANES), F32)
    for h in range(HEADS):
        bias_row = jnp.where(lane_head == h, tb_ref[h], bias_row)

    acc_ref[...] = jnp.zeros_like(acc_ref)
    row_ref[...] = jnp.zeros_like(row_ref)
    bkv_ref[...] = jnp.zeros_like(bkv_ref)

    def project(s, _):
        xhat, _r = stats(state_ref[s].astype(F32))
        normed = (xhat * again).astype(BF)
        normed_ref[s, HALO : HALO + atoms] = normed
        both = dot(normed, wp_ref[...]).astype(BF)
        q_ref[s] = both[:, :width]
        kv_ref[s, HALO : HALO + atoms] = both[:, width:]
        return 0

    lax.fori_loop(0, samples, project, 0)

    pl.semaphore_wait(barrier, A + S - 2)
    edges = [
        remote(state_ref.at[:, pl.ds(atoms - HALO, HALO), :], edge_ref.at[0], esend.at[0], erecv.at[0], (me_s, right)),
        remote(state_ref.at[:, pl.ds(0, HALO), :], edge_ref.at[1], esend.at[1], erecv.at[1], (me_s, left)),
        remote(qid_ref.at[pl.ds(windows - near, near)], eid_ref.at[0], esend.at[2], erecv.at[2], (me_s, right)),
        remote(qid_ref.at[pl.ds(0, near)], eid_ref.at[1], esend.at[3], erecv.at[3], (me_s, left)),
    ]
    for copy in edges:
        copy.start()

    def columns(rows):
        count = rows.shape[0]
        full = jnp.concatenate([rows.astype(F32), jnp.zeros((LANES - count, LANES), F32)], axis=0)
        turned = full.T
        return [jnp.broadcast_to(turned[:QWIN, j : j + 1], (QWIN, LANES)) for j in range(count)]

    for j, column in enumerate(columns(qid_ref[:, 0, :])):
        kid_ref[HALO + j * QWIN : HALO + (j + 1) * QWIN, :] = column

    def masks(w):
        base = pl.multiple_of(w * QWIN, QWIN)
        kid = kid_ref[pl.ds(base, KWIN), :]
        same = (kid == qid_ref[w][0:1].astype(F32)).astype(F32)
        same_ref[w] = same
        mask = jnp.where(kid > 0.0, same * bias_row, -1e30)
        mask_ref[w] = mask
        return mask

    def spread(rows):
        return jnp.concatenate([rows] * HEADS, axis=0) * head_b

    def gather_heads(value):
        return jnp.sum((value * head_f).reshape(HEADS, QWIN, width), axis=0)

    def attend_at(w):
        base = pl.multiple_of(w * QWIN, QWIN)
        mask = masks(w)
        for s in range(samples):
            keys = kv_ref[s, pl.ds(base, KWIN), :width]
            vals = kv_ref[s, pl.ds(base, KWIN), width:]
            turn_ref[s] = spread(q_ref[s, pl.ds(base, QWIN), :]).T
            score = dot(keys, turn_ref[s]) * scale + mask
            weight = jnp.exp(score - jnp.max(score, axis=0, keepdims=True))
            prob = (weight * (1.0 / jnp.sum(weight, axis=0, keepdims=True))).astype(BF)
            p_ref[s, w] = prob
            att_ref[s, pl.ds(base, QWIN), :] = gather_heads(dot_tn(prob, vals)).astype(BF)

    def attend(w, _):
        attend_at(w)
        return 0

    lax.fori_loop(near, windows - near, attend, 0)

    for copy in edges:
        copy.wait()
    has_before = (me_a > 0).astype(F32)
    has_after = (me_a < A - 1).astype(F32)
    for side, has in ((0, has_before), (1, has_after)):
        cols = jnp.concatenate(columns(eid_ref[side, :, 0, :]), axis=0) * has
        if side == 0:
            kid_ref[:HALO, :] = cols[near * QWIN - HALO :]
        else:
            kid_ref[HALO + atoms :, :] = cols[:HALO]

    def project_edge(s, _):
        both_edges = jnp.concatenate([edge_ref[0, s], edge_ref[1, s]], axis=0)
        xhat, _r = stats(both_edges.astype(F32))
        normed = (xhat * again).astype(BF)
        normed_ref[s, :HALO] = normed[:HALO]
        normed_ref[s, HALO + atoms :] = normed[HALO:]
        both = dot(normed, wp_ref[:, width:]).astype(BF)
        kv_ref[s, :HALO] = both[:HALO]
        kv_ref[s, HALO + atoms :] = both[HALO:]
        return 0

    lax.fori_loop(0, samples, project_edge, 0)

    def attend_edge(i, _):
        attend_at(jnp.where(i < near, i, windows - 2 * near + i))
        return 0

    lax.fori_loop(0, 2 * near, attend_edge, 0)

    def transit(s, _):
        state = state_ref[s].astype(F32)
        att = att_ref[s]
        residual = (state + dot(att, wo_ref[...])).astype(BF).astype(F32)
        xhat, rstd = stats(residual)
        tin = (xhat * tgain).astype(BF)
        both = dot(tin, wt_ref[...])
        gate, up = both[:, :TRANS], both[:, TRANS:]
        sig = 1.0 / (1.0 + jnp.exp(-gate))
        silu = gate * sig
        gated = (silu * up).astype(BF)
        out_ref[s] = (residual + dot(gated, wr_ref[...])).astype(BF)
        cot = cot_ref[s]
        acc_ref[5:7] += dot_tn(gated, cot).reshape(2, LANES, LANES)
        bg = dot_nt(cot, wr_ref[...])
        back_gate = (bg * up * sig * (1.0 + gate * (1.0 - sig))).astype(BF)
        back_up = (bg * silu).astype(BF)
        bh = jnp.concatenate([back_gate, back_up], axis=1)
        gt = dot_tn(tin, bh)
        for j in range(4):
            acc_ref[1 + j] += gt[:, j * LANES : (j + 1) * LANES]
        bt = dot_nt(bh, wt_ref[...])
        row_ref[1:2] += jnp.sum(bt * xhat, axis=0, keepdims=True)
        bres = cot.astype(F32) + norm_back(bt, xhat, rstd, tgain)
        bres_ref[s] = bres
        b16 = bres.astype(BF)
        acc_ref[0] += dot_tn(att, b16)
        batt_ref[s] = dot_nt(b16, wo_ref[...]).astype(BF)
        return 0

    lax.fori_loop(0, samples, transit, 0)

    class Reduce:
        def __init__(self, send, in1, mid, in2, full, sems):
            self.send, self.in1, self.mid, self.in2, self.full, self.sems = send, in1, mid, in2, full, sems
            self.started = []

        def over_atom(self, src_of, dst_of, k):
            copies = []
            for d in range(1, A):
                peer = lax.rem(me_a + d, A)
                copy = remote(src_of(peer), dst_of(d), self.sems.at[k, 0, d - 1], self.sems.at[k, 1, d - 1], (me_s, peer))
                copy.start()
                copies.append(copy)
            self.started += copies
            return copies

        def over_samp(self, src_of, dst_of, k):
            copies = []
            for d in range(1, S):
                peer = lax.rem(me_s + d, S)
                copy = remote(src_of(peer), dst_of(d), self.sems.at[k, 0, d - 1], self.sems.at[k, 1, d - 1], (peer, me_a))
                copy.start()
                copies.append(copy)
            self.started += copies
            return copies

        def step1(self):
            self.c1 = self.over_atom(lambda p: self.send.at[p], lambda d: self.in1.at[d - 1], 0)

        def step2(self):
            total = self.send[me_a].astype(F32)
            for d in range(1, A):
                self.c1[d - 1].wait_recv()
                total = total + self.in1[d - 1].astype(F32)
            self.mid[...] = total.astype(BF)
            self.c2 = self.over_samp(lambda p: self.mid.at[p], lambda d: self.in2.at[d - 1], 1)

        def step3(self):
            mine = self.mid[me_s].astype(F32)
            for d in range(1, S):
                self.c2[d - 1].wait_recv()
                mine = mine + self.in2[d - 1].astype(F32)
            self.full[me_a, me_s] = mine.astype(BF)
            self.over_samp(lambda p: self.full.at[me_a, me_s], lambda d: self.full.at[me_a, me_s], 2)

        def step4(self):
            for d in range(1, S):
                src = lax.rem(me_s + S - d, S)
                ref = self.full.at[me_a, src]
                remote(ref, ref, self.sems.at[2, 0, d - 1], self.sems.at[2, 1, d - 1], (src, me_a)).wait_recv()
            self.over_atom(lambda p: self.full.at[me_a], lambda d: self.full.at[me_a], 3)

        def step5(self):
            for d in range(1, A):
                src = lax.rem(me_a + A - d, A)
                ref = self.full.at[src]
                remote(ref, ref, self.sems.at[3, 0, d - 1], self.sems.at[3, 1, d - 1], (me_s, src)).wait_recv()
            for copy in self.started:
                copy.wait_send()

    def pack(dst, parts):
        rows = A * S * dst.shape[2]
        used = sum(p.shape[0] for p in parts)
        if rows > used:
            parts = parts + [jnp.zeros((rows - used, LANES), F32)]
        dst[...] = jnp.concatenate(parts, axis=0).reshape(dst.shape).astype(BF)

    red_a = Reduce(send_a, in1_a, mid_a, in2_a, all_a, sems_a)
    red_b = Reduce(send_b, in1_b, mid_b, in2_b, all_b, sems_b)

    pack(send_a, [acc_ref[j] for j in range(7)])
    red_a.step1()

    def attend_back(w, _):
        base = pl.multiple_of(w * QWIN, QWIN)
        total = jnp.zeros((KWIN, LANES), F32)
        for s in range(samples):
            keys = kv_ref[s, pl.ds(base, KWIN), :width]
            vals = kv_ref[s, pl.ds(base, KWIN), width:]
            qs = spread(q_ref[s, pl.ds(base, QWIN), :])
            bo = spread(batt_ref[s, pl.ds(base, QWIN), :])
            prob = p_ref[s, w]
            pf = prob.astype(F32)
            turn_ref[s] = bo.T
            bp = dot(vals, turn_ref[s])
            pbp = pf * bp
            bs = pbp - pf * jnp.sum(pbp, axis=0, keepdims=True)
            total = total + bs
            b16 = (bs * scale).astype(BF)
            bq_ref[s, pl.ds(base, QWIN), :] = gather_heads(dot_tn(b16, keys)).astype(BF)
            bkv_ref[s, pl.ds(base, KWIN), :width] += dot(b16, qs)
            bkv_ref[s, pl.ds(base, KWIN), width:] += dot(prob, bo)
        row_ref[2:3] += jnp.sum(total * same_ref[w], axis=0, keepdims=True)
        return 0

    half = windows // 2
    lax.fori_loop(0, half, attend_back, 0)
    red_a.step2()
    lax.fori_loop(half, windows, attend_back, 0)
    red_a.step3()

    def finish(s, _):
        normed = normed_ref[s]
        bkv = bkv_ref[s].astype(BF)
        bq = bq_ref[s]
        acc_ref[7] += dot_tn(normed[HALO : HALO + atoms], bq)
        gkv = dot_tn(normed, bkv)
        acc_ref[8] += gkv[:, :LANES]
        acc_ref[9] += gkv[:, LANES:]
        back = dot_nt(bkv, wp_ref[:, width:])
        own = back[HALO : HALO + atoms] + dot_nt(bq, wp_ref[:, :width])
        xhat, _r = stats(state_ref[s].astype(F32))
        xb, _r = stats(edge_ref[0, s].astype(F32))
        xa, _r = stats(edge_ref[1, s].astype(F32))
        halo_before = back[:HALO]
        halo_after = back[HALO + atoms :]
        row_ref[0:1] += (
            jnp.sum(own * xhat, axis=0, keepdims=True)
            + jnp.sum(halo_before * xb, axis=0, keepdims=True)
            + jnp.sum(halo_after * xa, axis=0, keepdims=True)
        )
        halo_ref[0, s] = halo_after.astype(BF)
        halo_ref[1, s] = halo_before.astype(BF)
        bnorm_ref[s] = own
        return 0

    lax.fori_loop(0, samples, finish, 0)

    pieces = [acc_ref[7 + j] for j in range(3)]
    for i in range(3):
        hi, lo = split_hi_lo(row_ref[i : i + 1])
        pieces += [hi.astype(F32), lo.astype(F32)]
    pieces[3:] = [jnp.concatenate(pieces[3:] + [jnp.zeros((10, LANES), F32)], axis=0)]
    pack(send_b, pieces)
    red_b.step1()
    rims = [
        remote(halo_ref.at[0], rim_ref.at[0], hsend.at[0], hrecv.at[0], (me_s, right)),
        remote(halo_ref.at[1], rim_ref.at[1], hsend.at[1], hrecv.at[1], (me_s, left)),
    ]
    for copy in rims:
        copy.start()
    red_a.step4()
    red_b.step2()
    for copy in rims:
        copy.wait()

    def close(s, _):
        xhat, rstd = stats(state_ref[s].astype(F32))
        own = bnorm_ref[s]
        top = own[:HALO] + rim_ref[0, s].astype(F32) * has_before
        bottom = own[atoms - HALO :] + rim_ref[1, s].astype(F32) * has_after
        back = jnp.concatenate([top, own[HALO : atoms - HALO], bottom], axis=0)
        sg_ref[s] = (bres_ref[s] + norm_back(back, xhat, rstd, again)).astype(BF)
        return 0

    lax.fori_loop(0, samples // 2, close, 0)
    red_b.step3()
    lax.fori_loop(samples // 2, samples, close, 0)
    red_b.step4()
    red_a.step5()
    ga_ref[...] = all_a[...]
    red_b.step5()
    gb_ref[...] = all_b[...]


def clip_kernel(ga_ref, gb_ref, out_in, sg_in, out_ref, sg_ref, gag_ref, gp_ref, go_ref, gb_out, gtg_ref, gt_ref, gr_ref):
    out_ref[...] = out_in[...]
    sg_ref[...] = sg_in[...]
    fa = ga_ref[...].astype(F32).reshape(-1, LANES)
    fb = gb_ref[...].astype(F32).reshape(-1, LANES)
    blocks = [fa[j * LANES : (j + 1) * LANES] for j in range(7)] + [fb[j * LANES : (j + 1) * LANES] for j in range(3)]
    rest = fb[3 * LANES : 3 * LANES + 6]
    rows = [rest[0:1] + rest[1:2], rest[2:3] + rest[3:4], rest[4:5] + rest[5:6]]
    lane = lax.broadcasted_iota(jnp.int32, (1, LANES), 1)
    bias = jnp.zeros((1, LANES), F32)
    for h in range(HEADS):
        part = jnp.sum(jnp.where(lane // QWIN == h, rows[2], 0.0), axis=1, keepdims=True)
        bias = bias + jnp.where(lane == h, part, 0.0)
    sq = blocks[0] * blocks[0]
    for b in blocks[1:]:
        sq = sq + b * b
    sq = jnp.sum(sq, axis=0, keepdims=True) + rows[0] * rows[0] + rows[1] * rows[1] + bias * bias
    squares = jnp.sum(sq, axis=1, keepdims=True)
    factor = CLIP_NORM / jnp.sqrt(squares + CLIP_NORM * CLIP_NORM)
    gag_ref[...] = rows[0] * factor
    gtg_ref[...] = rows[1] * factor
    gb_out[...] = bias * factor
    go_ref[...] = blocks[0] * factor
    for j in range(4):
        gt_ref[:, j * LANES : (j + 1) * LANES] = blocks[1 + j] * factor
    for j in range(2):
        gr_ref[j * LANES : (j + 1) * LANES, :] = blocks[5 + j] * factor
    for j in range(3):
        gp_ref[:, j * LANES : (j + 1) * LANES] = blocks[7 + j] * factor


def on_device(A, S, atom_state, atom_token, window_valid, attend_gain, project_weight, output_weight,
              token_bias, transit_gain, transit_weight, return_weight, cotangent):
    samples, atoms, width = atom_state.shape
    windows = window_valid.shape[0]
    ext = atoms + 2 * HALO
    near = -(-HALO // QWIN)
    slots = lax.broadcasted_iota(jnp.int32, (windows, QWIN), 1)
    ids = jnp.where(slots < window_valid[:, None], atom_token.reshape(windows, QWIN) + 1, 0)
    qid = jnp.broadcast_to(jnp.tile(ids, (1, HEADS))[:, None, :], (windows, 8, LANES))
    again = attend_gain.reshape(1, width)
    tgain = transit_gain.reshape(1, width)
    shards = A * S
    per_a = -(-7 * LANES // (shards * 16)) * 16
    per_b = -(-(3 * LANES + 16) // (shards * 16)) * 16
    vm = pl.BlockSpec(memory_space=pltpu.VMEM)
    sds = jax.ShapeDtypeStruct
    act = (samples, atoms, width)
    dma = pltpu.SemaphoreType.DMA
    top = max(A, S) - 1

    def buffers(per):
        return [
            pltpu.VMEM((A, S, per, LANES), BF),
            pltpu.VMEM((S, per, LANES), BF),
            pltpu.VMEM((A - 1, S, per, LANES), BF),
            pltpu.VMEM((S - 1, per, LANES), BF),
            pltpu.VMEM((A, S, per, LANES), BF),
        ]

    block_out, sg, ga, gb = pl.pallas_call(
        functools.partial(mega_kernel, A, S),
        out_shape=(sds(act, BF), sds(act, BF), sds((A, S, per_a, LANES), BF), sds((A, S, per_b, LANES), BF)),
        in_specs=[vm] * 6 + [pl.BlockSpec(memory_space=pltpu.SMEM)] + [vm] * 3,
        out_specs=(vm,) * 4,
        scratch_shapes=[
            pltpu.VMEM((2, samples, HALO, width), BF),
            pltpu.VMEM((2, near, 8, LANES), jnp.int32),
            pltpu.VMEM((ext, LANES), F32),
            pltpu.VMEM((samples, ext, width), BF),
            pltpu.VMEM(act, BF),
            pltpu.VMEM((samples, ext, 2 * width), BF),
            pltpu.VMEM((samples, windows, KWIN, LANES), BF),
            pltpu.VMEM(act, BF),
            pltpu.VMEM(act, BF),
            pltpu.VMEM(act, BF),
            pltpu.VMEM((samples, ext, 2 * width), F32),
            pltpu.VMEM((windows, KWIN, LANES), F32),
            pltpu.VMEM((windows, KWIN, LANES), F32),
            pltpu.VMEM((10, LANES, LANES), F32),
            pltpu.VMEM((8, LANES), F32),
            pltpu.VMEM(act, F32),
            pltpu.VMEM(act, F32),
            pltpu.VMEM((2, samples, HALO, width), BF),
            pltpu.VMEM((2, samples, HALO, width), BF),
        ]
        + buffers(per_a)
        + buffers(per_b)
        + [dma((4,)), dma((4,)), dma((2,)), dma((2,)), dma((4, 2, top)), dma((4, 2, top)),
           pltpu.VMEM((samples, HEADS * QWIN, LANES), BF)],
        compiler_params=pltpu.CompilerParams(collective_id=0, has_side_effects=True),
        name="block",
    )(atom_state, cotangent, qid, again, project_weight, output_weight, token_bias, tgain,
      transit_weight, return_weight)
    block_out, sg, gag, gp, go, gbias, gtg, gt, gr = pl.pallas_call(
        clip_kernel,
        out_shape=(sds(act, BF), sds(act, BF), sds((1, width), F32), sds((width, 3 * width), F32),
                   sds((width, width), F32), sds((1, LANES), F32), sds((1, width), F32),
                   sds((width, 2 * TRANS), F32), sds((TRANS, width), F32)),
        in_specs=[vm] * 4,
        out_specs=(vm,) * 9,
        name="clip",
    )(ga, gb, block_out, sg)
    return (block_out, sg, gag.reshape(width), gp, go, gbias[0, :HEADS], gtg.reshape(width), gt, gr)


def solution(mesh):
    A, S = mesh.shape["atom"], mesh.shape["samp"]
    act = P("samp", "atom", None)
    return jax.shard_map(
        functools.partial(on_device, A, S),
        mesh=mesh,
        in_specs=(act, P("atom"), P("atom"), P(), P(), P(), P(), P(), P(), P(), act),
        out_specs=(act, act, P(), P(), P(), P(), P(), P(), P()),
        check_vma=False,
    )
```
